128 devices in a mesh: sec: 64 (over x, y, z), node: 2 (over core).
Axes of the slice: x: 4, y: 4, z: 4, core: 2. Of those that a mesh axis runs over, the one named last changes fastest.
Arguments:
- env_blocks: bfloat16 [2, 24576, 128, 128], P('node', 'sec'), may hold values from -10 to 10, as said below
- iso_blocks: bfloat16 [2, 24576, 128, 128], P('node', 'sec'), may hold values from -6 to 6
- joined_sector: int32 [2, 24576], P('node', 'sec'), may hold values from 0 to 63, as said below
- owner_map: int32 [2, 64], P('node'), may hold values from 0 to 63, each once within a row
- live_pairs: int32 [2, 64], P('node', 'sec'), may hold values from 1 to 384, as said below
Outputs:
- environment: float32 [2, 64, 128, 128], P('node', 'sec')
The draws below stay inside these ranges and needn't reach their ends.
Inputs may be any that keep to these rules, and one draw needn't show every extreme that they name: `env_blocks`: each block is symmetric. `joined_sector`: slot p belongs to tree node k = p // 3072 of its group, and its sector is one of that node's sectors k * 8 to k * 8 + 7. `owner_map`: each row names every index once. `live_pairs`: in every group some index of sec has all 384 slots live.
All inputs are finite; a program needn't handle non-finite values.
Results may differ from the reference program's by a relative error of at most 0.0003.
Values sent between devices are 32-bit elements; how exact they have to be, the bound alone decides.
No kernel may reach another device: no remote copies, remote signals or barrier semaphores. Data moves between devices by JAX's collectives and lax.ppermute only.
A program may use at most 128 MiB of HBM per device.

```python
import math
import jax
import jax.numpy as jnp
from jax import lax

R = 128
DC = 128
SECTORS_NODE = 8
PAIRS_DEV = 384
NODES = 2
SECTORS = 64
PAIRS = 24576


def draw_env_blocks(key, part):
    base = jax.random.truncated_normal(jax.random.fold_in(key, 11), -4.0, 4.0, (NODES, PAIRS, R, R), jnp.float32)
    blocks = (base + jnp.swapaxes(base, -1, -2)) * (0.7 / math.sqrt(R)) + jnp.eye(R, dtype=jnp.float32)
    return blocks.astype(jnp.bfloat16)


def draw_iso_blocks(key, part):
    tree_count = PAIRS // (PAIRS_DEV * SECTORS_NODE)
    per_tree = PAIRS_DEV * SECTORS_NODE
    shared = jax.random.truncated_normal(jax.random.fold_in(key, 41), -4.0, 4.0, (NODES, tree_count, 1, R, DC), jnp.float32)
    logs = jax.random.uniform(jax.random.fold_in(key, 42), (NODES, tree_count, 1, 1, DC), jnp.float32, math.log(0.4), math.log(4.0))
    column_scales = jnp.exp(logs)
    own = jax.random.truncated_normal(jax.random.fold_in(key, 44), -4.0, 4.0, (NODES, tree_count, per_tree, R, DC), jnp.float32)
    mixed = 0.8 * shared + 0.6 * own
    blocks = mixed * column_scales * (1.0 / math.sqrt(R))
    return blocks.reshape(NODES, PAIRS, R, DC).astype(jnp.bfloat16)


def draw_joined_sector(key, part):
    first_draw = jax.random.randint(jax.random.fold_in(key, 31), (NODES, PAIRS), 0, SECTORS_NODE)
    second_draw = jax.random.randint(jax.random.fold_in(key, 32), (NODES, PAIRS), 0, SECTORS_NODE)
    within = jnp.minimum(first_draw, second_draw)
    slots = jnp.arange(PAIRS, dtype=jnp.int32)[None, :]
    tree_node = slots // (PAIRS_DEV * SECTORS_NODE)
    return (tree_node * SECTORS_NODE + within).astype(jnp.int32)


def draw_live_pairs(key, part):
    first_draw = jax.random.randint(jax.random.fold_in(key, 21), (NODES, SECTORS), 1, PAIRS_DEV + 1)
    second_draw = jax.random.randint(jax.random.fold_in(key, 22), (NODES, SECTORS), 1, PAIRS_DEV + 1)
    counts = jnp.minimum(first_draw, second_draw)
    chosen = jax.random.randint(jax.random.fold_in(key, 23), (NODES, 1), 0, SECTORS)
    places = jnp.arange(SECTORS, dtype=jnp.int32)[None, :]
    return jnp.where(places == chosen, PAIRS_DEV, counts).astype(jnp.int32)


def setup_inputs(seed: int = 0) -> dict:
    key_list = jax.random.split(jax.random.key(seed), 6)
    return {
        "env_blocks": draw_env_blocks(jax.random.fold_in(key_list[5], 71), 0),
        "iso_blocks": draw_iso_blocks(jax.random.fold_in(key_list[5], 71), 0),
        "joined_sector": draw_joined_sector(jax.random.fold_in(key_list[5], 71), 0),
        "owner_map": jax.vmap(lambda own: jax.random.permutation(own, SECTORS))(jax.random.split(key_list[3], NODES)).reshape((NODES, SECTORS)).astype(jnp.int32),
        "live_pairs": draw_live_pairs(jax.random.fold_in(key_list[5], 71), 0),
    }


def reference(env_blocks, iso_blocks, joined_sector, owner_map, live_pairs):
    hermitians = []
    for node_index in range(NODES):
        targets_all = owner_map[node_index][joined_sector[node_index]].astype(jnp.int32)

        def one_source(partial_value, source, node_index=node_index, targets_all=targets_all):
            first_pair = (source * PAIRS_DEV).astype(jnp.int32)
            zero_index = jnp.zeros((), jnp.int32)
            node_start = (zero_index + node_index).astype(jnp.int32)
            blocks = lax.dynamic_slice(env_blocks, (node_start, first_pair, zero_index, zero_index), (1, PAIRS_DEV, R, R))[0].astype(jnp.float32)
            weights = lax.dynamic_slice(iso_blocks, (node_start, first_pair, zero_index, zero_index), (1, PAIRS_DEV, R, DC))[0].astype(jnp.float32)
            product = jnp.einsum('prk,pkc->prc', blocks, weights, precision=lax.Precision.HIGHEST).astype(jnp.bfloat16)
            sandwich = jnp.einsum('prc,prd->pcd', weights, product.astype(jnp.float32), precision=lax.Precision.HIGHEST)
            living = jnp.arange(PAIRS_DEV, dtype=jnp.int32) < live_pairs[node_index, source]
            sandwich = jnp.where(living[:, None, None], sandwich, jnp.zeros((), jnp.float32))
            targets = lax.dynamic_slice_in_dim(targets_all, first_pair, PAIRS_DEV, 0)
            return (partial_value.at[targets].add(sandwich), None)
        zero_sums = jnp.zeros((SECTORS, DC, DC), jnp.float32)
        partial_value, unused = lax.scan(one_source, zero_sums, jnp.arange(SECTORS, dtype=jnp.int32))
        hermitian = jnp.triu(partial_value) + jnp.swapaxes(jnp.triu(partial_value, 1), 1, 2)
        hermitians.append(hermitian)
    stacked = jnp.stack(hermitians, axis=0)
    grand_total = jnp.sum(stacked * stacked)
    factor = lax.rsqrt(grand_total / (NODES * SECTORS * DC * DC) + 1e-06)
    return stacked * factor
```

```python
import functools

import jax
import jax.numpy as jnp
from jax import lax
from jax.experimental import pallas as pl
from jax.experimental.pallas import tpu as pltpu
from jax.sharding import Mesh
from jax.sharding import PartitionSpec as P

SEC = ("x", "y_hi", "y_lo", "z")
ALL = SEC + ("node",)
FAMILY = ("y_lo", "z", "node")
LOCAL = 8
DC = 128
HALF = 64
SLOTS = 384
CHUNK = 32
CHUNKS = SLOTS // CHUNK
PIECE = 40
F32 = jnp.float32


def rows_and_lanes(rows):
    row = lax.broadcasted_iota(jnp.int32, (rows, DC), 0)
    lane = lax.broadcasted_iota(jnp.int32, (rows, DC), 1)
    return row, lane


def partial_sums(live_ref, joined_ref, owner_ref, env, iso, out_ref, e_buf, w_buf, acc, e_sem, w_sem):
    live = live_ref[0, 0]
    chunks = (live + CHUNK - 1) // CHUNK

    def copies(chunk):
        here = pl.ds(chunk * CHUNK, CHUNK)
        return (
            pltpu.make_async_copy(env.at[0, here], e_buf.at[here], e_sem.at[chunk]),
            pltpu.make_async_copy(iso.at[0, here], w_buf.at[here], w_sem.at[chunk]),
        )

    def start(chunk, carry):
        for copy in copies(chunk):
            copy.start()
        return carry

    lax.fori_loop(0, chunks, start, 0)
    acc[...] = jnp.zeros_like(acc)

    def add_chunk(chunk, carry):
        for copy in copies(chunk):
            copy.wait()
        for u in range(CHUNK):
            slot = chunk * CHUNK + u
            weights = w_buf[slot]
            product = jnp.dot(e_buf[slot], weights, preferred_element_type=F32).astype(jnp.bfloat16)
            term = lax.dot_general(
                weights, product, (((0,), (0,)), ((), ())), preferred_element_type=F32
            )
            sector = jnp.where(slot < live, joined_ref[0, slot] & (LOCAL - 1), LOCAL)
            acc[sector] = acc[sector] + term
        return carry

    lax.fori_loop(0, chunks, add_chunk, 0)

    row, lane = rows_and_lanes(HALF)
    row8, lane8 = rows_and_lanes(8)
    family = 2 * lax.axis_index("x") + lax.axis_index("y_hi")
    packed, diagonals = [], []
    for j in range(LOCAL):
        top, bottom = acc[j, :HALF], acc[j, HALF:]
        turned = pltpu.roll(acc[j].T[HALF:], HALF, 1)
        packed.append(jnp.where(lane >= row, top, turned))
        diagonal = jnp.sum(jnp.where(lane == row + HALF, bottom, 0.0), axis=0, keepdims=True)
        owner = owner_ref[0, LOCAL * family + j].astype(F32)
        diagonals.append(jnp.where(lane8[:1] < HALF, owner, diagonal))
    diagonal_tile = jnp.concatenate(diagonals, axis=0)
    for v in range(8):
        rows = slice(8 * v, 8 * v + 8)
        for pair in range(LOCAL // 2):
            even, odd = packed[2 * pair][rows], packed[2 * pair + 1][rows]
            out_ref[2 * v, 8 * pair : 8 * pair + 8] = jnp.where(row8 < 4, even, odd)
            out_ref[2 * v + 1, 8 * pair : 8 * pair + 8] = jnp.where(row8 < 4, odd, even)
        out_ref[2 * v, 32:40] = diagonal_tile
        out_ref[2 * v + 1, 32:40] = diagonal_tile


def reduce_pieces(got_ref, out_ref):
    v = lax.axis_index("y_lo") * 4 + lax.axis_index("z")
    h = lax.axis_index("node")
    row, lane = rows_and_lanes(8)
    weight = jnp.where((lane < HALF) & (lane == row + 8 * v), 1.0, 2.0)
    first = HALF + 8 * v + 4 * h
    mine = (lane >= first) & (lane < first + 4)
    squares = jnp.zeros((8, DC), F32)
    summed = []
    for n in range(2):
        tiles = []
        for t in range(5):
            rows = slice(8 * t, 8 * t + 8)
            total = got_ref[n, rows]
            for source in range(1, 8):
                total = total + got_ref[2 * source + n, rows]
            tiles.append(total)
            squares = squares + jnp.where(mine, total * total, 0.0) if t == 4 else squares + weight * (total * total)
        summed.append(tiles)
    part = jnp.sum(squares)
    out_ref[...] = jnp.zeros_like(out_ref)
    out_ref[:, 0, 512:640] = jnp.full((128, DC), part, F32)
    for n in range(2):
        extra = summed[n][4]
        owners = (extra[:, :1] * 0.125).astype(jnp.int32)
        for j in range(LOCAL):
            slot = 2 * owners[j, 0] + n
            tile = summed[n][j // 2]
            low, high = tile[:4], tile[4:]
            mine4 = jnp.where(h == j % 2, low, high)
            for r in range(4):
                out_ref[slot, :, DC * r : DC * (r + 1)] = mine4[r : r + 1]
            out_ref[slot, :, 512:640] = jnp.where(lane[:1] < HALF, part, extra[j : j + 1])


def unpack(owner_ref, got_ref, out_ref, rows_buf):
    sec = (
        (lax.axis_index("x") * 2 + lax.axis_index("y_hi")) * 2 + lax.axis_index("y_lo")
    ) * 4 + lax.axis_index("z")
    sector = jnp.int32(0)
    for d in range(64):
        sector = jnp.where(owner_ref[0, d] == sec, d, sector)
    base = 16 * (sector // LOCAL)
    odd = sector % 2
    for v in range(8):
        for half in range(2):
            source = base + 2 * v + jnp.where(odd == 0, half, 1 - half)
            for r in range(4):
                rows_buf[8 * v + 4 * half + r : 8 * v + 4 * half + r + 1, :] = got_ref[
                    source, :, DC * r : DC * (r + 1)
                ]
    rows_buf[HALF:, :] = jnp.zeros((HALF, DC), F32)
    extra = got_ref[base, :, 512:640]
    total = jnp.sum(got_ref[:, 0, 512:640], axis=0, keepdims=True)[:, :1]
    factor = lax.rsqrt(total / (2 * 64 * DC * DC) + 1e-06)
    row, lane = rows_and_lanes(HALF)
    packed = rows_buf[:HALF, :]
    turned = rows_buf[...].T
    top = jnp.where(lane >= row, packed, turned[:HALF])
    inner = pltpu.roll(jnp.where(lane < row, packed, turned[:HALF]), HALF, 1)
    inner = jnp.where(lane == row + HALF, extra, inner)
    bottom = jnp.where(lane < HALF, turned[HALF:], inner)
    out_ref[0, 0, :HALF, :] = top * factor
    out_ref[0, 0, HALF:, :] = bottom * factor


def body(env_blocks, iso_blocks, joined_sector, owner_map, live_pairs):
    smem = pl.BlockSpec(memory_space=pltpu.SMEM)
    vmem = pl.BlockSpec(memory_space=pltpu.VMEM)
    hbm = pl.BlockSpec(memory_space=pl.ANY)
    pieces = pl.pallas_call(
        partial_sums,
        in_specs=[smem, smem, smem, hbm, hbm],
        out_specs=vmem,
        out_shape=jax.ShapeDtypeStruct((16, PIECE, DC), F32),
        scratch_shapes=[
            pltpu.VMEM((SLOTS, DC, DC), jnp.bfloat16),
            pltpu.VMEM((SLOTS, DC, DC), jnp.bfloat16),
            pltpu.VMEM((LOCAL + 1, DC, DC), F32),
            pltpu.SemaphoreType.DMA((CHUNKS,)),
            pltpu.SemaphoreType.DMA((CHUNKS,)),
        ],
        compiler_params=pltpu.CompilerParams(vmem_limit_bytes=48 << 20),
        name="partial_sums",
    )(live_pairs, joined_sector, owner_map, env_blocks, iso_blocks)
    pieces = lax.all_to_all(pieces, FAMILY, 0, 0, tiled=True)
    slots = pl.pallas_call(
        reduce_pieces,
        in_specs=[vmem],
        out_specs=vmem,
        out_shape=jax.ShapeDtypeStruct((128, 1, 640), F32),
        name="reduce_pieces",
    )(pieces)
    slots = lax.all_to_all(slots, ALL, 0, 0, tiled=True)
    return pl.pallas_call(
        unpack,
        in_specs=[smem, vmem],
        out_specs=vmem,
        out_shape=jax.ShapeDtypeStruct((1, 1, DC, DC), F32),
        scratch_shapes=[pltpu.VMEM((DC, DC), F32)],
        name="unpack",
    )(owner_map, slots)


def solution(mesh):
    split = Mesh(mesh.devices.reshape(4, 2, 2, 4, mesh.shape["node"]), ALL)
    placed = (
        P("node", SEC, None, None),
        P("node", SEC, None, None),
        P("node", SEC),
        P("node", None),
        P("node", SEC),
    )
    return jax.shard_map(
        body, mesh=split, in_specs=placed, out_specs=P("node", SEC, None, None), check_vma=False
    )
```

```python
import functools

import jax
import jax.numpy as jnp
from jax import lax
from jax.experimental import pallas as pl
from jax.experimental.pallas import tpu as pltpu
from jax.sharding import Mesh
from jax.sharding import PartitionSpec as P

SEC = ("x", "y_hi", "y_lo", "z")
ALL = SEC + ("node",)
FAMILY = ("y_lo", "z", "node")
LOCAL = 8
DC = 128
HALF = 64
SLOTS = 384
CHUNK = 64
CHUNKS = SLOTS // CHUNK
PIECE = 40
F32 = jnp.float32


def rows_and_lanes(rows):
    row = lax.broadcasted_iota(jnp.int32, (rows, DC), 0)
    lane = lax.broadcasted_iota(jnp.int32, (rows, DC), 1)
    return row, lane


def partial_sums(
    live_hbm, joined_hbm, owner_hbm, env, iso, out_ref, sector_ref,
    e_buf, w_buf, acc, live_ref, joined_ref, owner_ref, e_sem, w_sem, small_sem,
):
    small = [
        pltpu.make_async_copy(source, target, small_sem.at[i])
        for i, (source, target) in enumerate(
            ((live_hbm, live_ref), (joined_hbm, joined_ref), (owner_hbm, owner_ref))
        )
    ]
    for copy in small:
        copy.start()

    def copies(chunk):
        here = pl.ds(chunk * CHUNK, CHUNK)
        return (
            pltpu.make_async_copy(env.at[0, here], e_buf.at[here], e_sem.at[chunk]),
            pltpu.make_async_copy(iso.at[0, here], w_buf.at[here], w_sem.at[chunk]),
        )

    def start(chunk, carry):
        for copy in copies(chunk):
            copy.start()
        return carry

    start(0, 0)
    acc[...] = jnp.zeros_like(acc)
    small[0].wait()
    live = live_ref[0, 0]
    chunks = (live + CHUNK - 1) // CHUNK
    lax.fori_loop(1, chunks, start, 0)
    small[1].wait()
    small[2].wait()
    sec = (
        (lax.axis_index("x") * 2 + lax.axis_index("y_hi")) * 2 + lax.axis_index("y_lo")
    ) * 4 + lax.axis_index("z")
    sector_ref[0, 0] = lax.fori_loop(
        0, 64, lambda d, found: jnp.where(owner_ref[0, d] == sec, d, found), jnp.int32(0)
    )

    def add_chunk(chunk, carry):
        for copy in copies(chunk):
            copy.wait()
        for u in range(CHUNK):
            slot = chunk * CHUNK + u
            weights = w_buf[slot]
            product = jnp.dot(e_buf[slot], weights, preferred_element_type=F32).astype(jnp.bfloat16)
            term = lax.dot_general(
                weights, product, (((0,), (0,)), ((), ())), preferred_element_type=F32
            )
            sector = jnp.where(slot < live, joined_ref[0, slot] & (LOCAL - 1), LOCAL)
            acc[sector] = acc[sector] + term
        return carry

    lax.fori_loop(0, chunks, add_chunk, 0)

    row, lane = rows_and_lanes(HALF)
    row8, lane8 = rows_and_lanes(8)
    family = 2 * lax.axis_index("x") + lax.axis_index("y_hi")
    packed, diagonals = [], []
    for j in range(LOCAL):
        top, bottom = acc[j, :HALF], acc[j, HALF:]
        turned = pltpu.roll(acc[j].T[HALF:], HALF, 1)
        packed.append(jnp.where(lane >= row, top, turned))
        diagonal = jnp.sum(jnp.where(lane == row + HALF, bottom, 0.0), axis=0, keepdims=True)
        owner = owner_ref[0, LOCAL * family + j].astype(F32)
        diagonals.append(jnp.where(lane8[:1] < HALF, owner, diagonal))
    diagonal_tile = jnp.concatenate(diagonals, axis=0)
    for v in range(8):
        rows = slice(8 * v, 8 * v + 8)
        for pair in range(LOCAL // 2):
            even, odd = packed[2 * pair][rows], packed[2 * pair + 1][rows]
            out_ref[2 * v, 8 * pair : 8 * pair + 8] = jnp.where(row8 < 4, even, odd)
            out_ref[2 * v + 1, 8 * pair : 8 * pair + 8] = jnp.where(row8 < 4, odd, even)
        out_ref[2 * v, 32:40] = diagonal_tile
        out_ref[2 * v + 1, 32:40] = diagonal_tile


def reduce_pieces(got_ref, out_ref):
    v = lax.axis_index("y_lo") * 4 + lax.axis_index("z")
    h = lax.axis_index("node")
    row, lane = rows_and_lanes(8)
    weight = jnp.where((lane < HALF) & (lane == row + 8 * v), 1.0, 2.0)
    first = HALF + 8 * v + 4 * h
    mine = (lane >= first) & (lane < first + 4)
    squares = jnp.zeros((8, DC), F32)
    summed = []
    for n in range(2):
        tiles = []
        for t in range(5):
            rows = slice(8 * t, 8 * t + 8)
            total = got_ref[n, rows]
            for source in range(1, 8):
                total = total + got_ref[2 * source + n, rows]
            tiles.append(total)
            squares = squares + jnp.where(mine, total * total, 0.0) if t == 4 else squares + weight * (total * total)
        summed.append(tiles)
    part = jnp.sum(squares)
    out_ref[...] = jnp.zeros_like(out_ref)
    out_ref[:, 0, 512:640] = jnp.full((128, DC), part, F32)
    for n in range(2):
        extra = summed[n][4]
        owners = (extra[:, :1] * 0.125).astype(jnp.int32)
        for j in range(LOCAL):
            slot = 2 * owners[j, 0] + n
            tile = summed[n][j // 2]
            low, high = tile[:4], tile[4:]
            mine4 = jnp.where(h == j % 2, low, high)
            for r in range(4):
                out_ref[slot, :, DC * r : DC * (r + 1)] = mine4[r : r + 1]
            out_ref[slot, :, 512:640] = jnp.where(lane[:1] < HALF, part, extra[j : j + 1])


def unpack(sector_ref, got_ref, out_ref, rows_buf):
    sector = sector_ref[0, 0]
    base = 16 * (sector // LOCAL)
    odd = sector % 2
    for v in range(8):
        for half in range(2):
            source = base + 2 * v + jnp.where(odd == 0, half, 1 - half)
            for r in range(4):
                rows_buf[8 * v + 4 * half + r : 8 * v + 4 * half + r + 1, :] = got_ref[
                    source, :, DC * r : DC * (r + 1)
                ]
    rows_buf[HALF:, :] = jnp.zeros((HALF, DC), F32)
    extra = got_ref[base, :, 512:640]
    total = jnp.sum(got_ref[:, 0, 512:640], axis=0, keepdims=True)[:, :1]
    factor = lax.rsqrt(total / (2 * 64 * DC * DC) + 1e-06)
    row, lane = rows_and_lanes(HALF)
    packed = rows_buf[:HALF, :]
    turned = rows_buf[...].T
    top = jnp.where(lane >= row, packed, turned[:HALF])
    inner = pltpu.roll(jnp.where(lane < row, packed, turned[:HALF]), HALF, 1)
    inner = jnp.where(lane == row + HALF, extra, inner)
    bottom = jnp.where(lane < HALF, turned[HALF:], inner)
    out_ref[0, 0, :HALF, :] = top * factor
    out_ref[0, 0, HALF:, :] = bottom * factor


def body(env_blocks, iso_blocks, joined_sector, owner_map, live_pairs):
    smem = pl.BlockSpec(memory_space=pltpu.SMEM)
    vmem = pl.BlockSpec(memory_space=pltpu.VMEM)
    hbm = pl.BlockSpec(memory_space=pltpu.HBM)
    pieces, sector = pl.pallas_call(
        partial_sums,
        in_specs=[hbm] * 5,
        out_specs=[vmem, smem],
        out_shape=[
            jax.ShapeDtypeStruct((16, PIECE, DC), F32),
            jax.ShapeDtypeStruct((1, 1), jnp.int32),
        ],
        scratch_shapes=[
            pltpu.VMEM((SLOTS, DC, DC), jnp.bfloat16),
            pltpu.VMEM((SLOTS, DC, DC), jnp.bfloat16),
            pltpu.VMEM((LOCAL + 1, DC, DC), F32),
            pltpu.SMEM((1, 1), jnp.int32),
            pltpu.SMEM((1, SLOTS), jnp.int32),
            pltpu.SMEM((1, 64), jnp.int32),
            pltpu.SemaphoreType.DMA((CHUNKS,)),
            pltpu.SemaphoreType.DMA((CHUNKS,)),
            pltpu.SemaphoreType.DMA((3,)),
        ],
        compiler_params=pltpu.CompilerParams(vmem_limit_bytes=48 << 20),
        name="partial_sums",
    )(live_pairs, joined_sector, owner_map, env_blocks, iso_blocks)
    pieces = lax.all_to_all(pieces, FAMILY, 0, 0, tiled=True)
    slots = pl.pallas_call(
        reduce_pieces,
        in_specs=[vmem],
        out_specs=vmem,
        out_shape=jax.ShapeDtypeStruct((128, 1, 640), F32),
        compiler_params=pltpu.CompilerParams(vmem_limit_bytes=8 << 20),
        name="reduce_pieces",
    )(pieces)
    slots = lax.all_to_all(slots, ALL, 0, 0, tiled=True)
    return pl.pallas_call(
        unpack,
        in_specs=[smem, vmem],
        out_specs=vmem,
        out_shape=jax.ShapeDtypeStruct((1, 1, DC, DC), F32),
        scratch_shapes=[pltpu.VMEM((DC, DC), F32)],
        compiler_params=pltpu.CompilerParams(vmem_limit_bytes=8 << 20),
        name="unpack",
    )(sector, slots)


def solution(mesh):
    split = Mesh(mesh.devices.reshape(4, 2, 2, 4, mesh.shape["node"]), ALL)
    placed = (
        P("node", SEC, None, None),
        P("node", SEC, None, None),
        P("node", SEC),
        P("node", None),
        P("node", SEC),
    )
    return jax.shard_map(
        body, mesh=split, in_specs=placed, out_specs=P("node", SEC, None, None), check_vma=False
    )
```

```python
import functools

import jax
import jax.numpy as jnp
from jax import lax
from jax.experimental import pallas as pl
from jax.experimental.pallas import tpu as pltpu
from jax.sharding import Mesh
from jax.sharding import PartitionSpec as P

SEC = ("x", "y_hi", "y_lo", "z")
ALL = SEC + ("node",)
FAMILY = ("y_lo", "z", "node")
LOCAL = 8
DC = 128
HALF = 64
SLOTS = 384
CHUNK = 64
CHUNKS = SLOTS // CHUNK
PIECE = 40
F32 = jnp.float32


def rows_and_lanes(rows):
    row = lax.broadcasted_iota(jnp.int32, (rows, DC), 0)
    lane = lax.broadcasted_iota(jnp.int32, (rows, DC), 1)
    return row, lane


def partial_sums(
    live_ref, joined_hbm, owner_hbm, env, iso, out_ref, sector_ref,
    e_buf, w_buf, acc, joined_ref, owner_ref, e_sem, w_sem, small_sem,
):
    small = [
        pltpu.make_async_copy(source, target, small_sem.at[i])
        for i, (source, target) in enumerate(
            ((joined_hbm, joined_ref), (owner_hbm, owner_ref))
        )
    ]
    for copy in small:
        copy.start()

    def copies(chunk):
        here = pl.ds(chunk * CHUNK, CHUNK)
        return (
            pltpu.make_async_copy(env.at[0, here], e_buf.at[here], e_sem.at[chunk]),
            pltpu.make_async_copy(iso.at[0, here], w_buf.at[here], w_sem.at[chunk]),
        )

    def start(chunk, carry):
        for copy in copies(chunk):
            copy.start()
        return carry

    live = live_ref[0, 0]
    chunks = (live + CHUNK - 1) // CHUNK
    lax.fori_loop(0, chunks, start, 0)
    acc[...] = jnp.zeros_like(acc)
    for copy in small:
        copy.wait()
    sec = (
        (lax.axis_index("x") * 2 + lax.axis_index("y_hi")) * 2 + lax.axis_index("y_lo")
    ) * 4 + lax.axis_index("z")
    sector = lax.fori_loop(
        0, 64, lambda d, found: jnp.where(owner_ref[0, d] == sec, d, found), jnp.int32(0)
    )
    sector_ref[...] = jnp.full((8, DC), sector, jnp.int32)

    def add_chunk(chunk, carry):
        for copy in copies(chunk):
            copy.wait()
        for u in range(CHUNK):
            slot = chunk * CHUNK + u
            weights = w_buf[slot]
            product = jnp.dot(e_buf[slot], weights, preferred_element_type=F32).astype(jnp.bfloat16)
            term = lax.dot_general(
                weights, product, (((0,), (0,)), ((), ())), preferred_element_type=F32
            )
            sector = jnp.where(slot < live, joined_ref[0, slot] & (LOCAL - 1), LOCAL)
            acc[sector] = acc[sector] + term
        return carry

    lax.fori_loop(0, chunks, add_chunk, 0)

    row, lane = rows_and_lanes(HALF)
    row8, lane8 = rows_and_lanes(8)
    family = 2 * lax.axis_index("x") + lax.axis_index("y_hi")
    packed, diagonals = [], []
    for j in range(LOCAL):
        top, bottom = acc[j, :HALF], acc[j, HALF:]
        turned = pltpu.roll(acc[j].T[HALF:], HALF, 1)
        packed.append(jnp.where(lane >= row, top, turned))
        diagonal = jnp.sum(jnp.where(lane == row + HALF, bottom, 0.0), axis=0, keepdims=True)
        owner = owner_ref[0, LOCAL * family + j].astype(F32)
        diagonals.append(jnp.where(lane8[:1] < HALF, owner, diagonal))
    diagonal_tile = jnp.concatenate(diagonals, axis=0)
    for v in range(8):
        rows = slice(8 * v, 8 * v + 8)
        for pair in range(LOCAL // 2):
            even, odd = packed[2 * pair][rows], packed[2 * pair + 1][rows]
            out_ref[2 * v, 8 * pair : 8 * pair + 8] = jnp.where(row8 < 4, even, odd)
            out_ref[2 * v + 1, 8 * pair : 8 * pair + 8] = jnp.where(row8 < 4, odd, even)
        out_ref[2 * v, 32:40] = diagonal_tile
        out_ref[2 * v + 1, 32:40] = diagonal_tile


def reduce_pieces(got_ref, out_ref):
    v = lax.axis_index("y_lo") * 4 + lax.axis_index("z")
    h = lax.axis_index("node")
    row, lane = rows_and_lanes(8)
    weight = jnp.where((lane < HALF) & (lane == row + 8 * v), 1.0, 2.0)
    first = HALF + 8 * v + 4 * h
    mine = (lane >= first) & (lane < first + 4)
    squares = jnp.zeros((8, DC), F32)
    summed = []
    for n in range(2):
        tiles = []
        for t in range(5):
            rows = slice(8 * t, 8 * t + 8)
            total = got_ref[n, rows]
            for source in range(1, 8):
                total = total + got_ref[2 * source + n, rows]
            tiles.append(total)
            squares = squares + jnp.where(mine, total * total, 0.0) if t == 4 else squares + weight * (total * total)
        summed.append(tiles)
    part = jnp.sum(squares)
    out_ref[...] = jnp.zeros_like(out_ref)
    out_ref[:, 0, 512:640] = jnp.full((128, DC), part, F32)
    for n in range(2):
        extra = summed[n][4]
        owners = (extra[:, :1] * 0.125).astype(jnp.int32)
        for j in range(LOCAL):
            slot = 2 * owners[j, 0] + n
            tile = summed[n][j // 2]
            low, high = tile[:4], tile[4:]
            mine4 = jnp.where(h == j % 2, low, high)
            for r in range(4):
                out_ref[slot, :, DC * r : DC * (r + 1)] = mine4[r : r + 1]
            out_ref[slot, :, 512:640] = jnp.where(lane[:1] < HALF, part, extra[j : j + 1])


def unpack(sector_ref, got_ref, out_ref, rows_buf):
    sector = sector_ref[:1, :1][0, 0]
    base = 16 * (sector // LOCAL)
    odd = sector % 2
    for v in range(8):
        for half in range(2):
            source = base + 2 * v + jnp.where(odd == 0, half, 1 - half)
            for r in range(4):
                rows_buf[8 * v + 4 * half + r : 8 * v + 4 * half + r + 1, :] = got_ref[
                    source, :, DC * r : DC * (r + 1)
                ]
    rows_buf[HALF:, :] = jnp.zeros((HALF, DC), F32)
    extra = got_ref[base, :, 512:640]
    total = jnp.sum(got_ref[:, 0, 512:640], axis=0, keepdims=True)[:, :1]
    factor = lax.rsqrt(total / (2 * 64 * DC * DC) + 1e-06)
    row, lane = rows_and_lanes(HALF)
    packed = rows_buf[:HALF, :]
    turned = rows_buf[...].T
    top = jnp.where(lane >= row, packed, turned[:HALF])
    inner = pltpu.roll(jnp.where(lane < row, packed, turned[:HALF]), HALF, 1)
    inner = jnp.where(lane == row + HALF, extra, inner)
    bottom = jnp.where(lane < HALF, turned[HALF:], inner)
    out_ref[0, 0, :HALF, :] = top * factor
    out_ref[0, 0, HALF:, :] = bottom * factor


def body(env_blocks, iso_blocks, joined_sector, owner_map, live_pairs):
    smem = pl.BlockSpec(memory_space=pltpu.SMEM)
    vmem = pl.BlockSpec(memory_space=pltpu.VMEM)
    hbm = pl.BlockSpec(memory_space=pltpu.HBM)
    pieces, sector = pl.pallas_call(
        partial_sums,
        in_specs=[smem] + [hbm] * 4,
        out_specs=[vmem, vmem],
        out_shape=[
            jax.ShapeDtypeStruct((16, PIECE, DC), F32),
            jax.ShapeDtypeStruct((8, DC), jnp.int32),
        ],
        scratch_shapes=[
            pltpu.VMEM((SLOTS, DC, DC), jnp.bfloat16),
            pltpu.VMEM((SLOTS, DC, DC), jnp.bfloat16),
            pltpu.VMEM((LOCAL + 1, DC, DC), F32),
            pltpu.SMEM((1, SLOTS), jnp.int32),
            pltpu.SMEM((1, 64), jnp.int32),
            pltpu.SemaphoreType.DMA((CHUNKS,)),
            pltpu.SemaphoreType.DMA((CHUNKS,)),
            pltpu.SemaphoreType.DMA((2,)),
        ],
        compiler_params=pltpu.CompilerParams(vmem_limit_bytes=48 << 20),
        name="partial_sums",
    )(
        live_pairs,
        pltpu.with_memory_space_constraint(joined_sector, pltpu.HBM),
        pltpu.with_memory_space_constraint(owner_map, pltpu.HBM),
        env_blocks,
        iso_blocks,
    )
    pieces = lax.all_to_all(pieces, FAMILY, 0, 0, tiled=True)
    slots = pl.pallas_call(
        reduce_pieces,
        in_specs=[vmem],
        out_specs=vmem,
        out_shape=jax.ShapeDtypeStruct((128, 1, 640), F32),
        compiler_params=pltpu.CompilerParams(vmem_limit_bytes=8 << 20),
        name="reduce_pieces",
    )(pieces)
    slots = lax.all_to_all(slots, ALL, 0, 0, tiled=True)
    return pl.pallas_call(
        unpack,
        in_specs=[vmem, vmem],
        out_specs=vmem,
        out_shape=jax.ShapeDtypeStruct((1, 1, DC, DC), F32),
        scratch_shapes=[pltpu.VMEM((DC, DC), F32)],
        compiler_params=pltpu.CompilerParams(vmem_limit_bytes=8 << 20),
        name="unpack",
    )(sector, slots)


def solution(mesh):
    split = Mesh(mesh.devices.reshape(4, 2, 2, 4, mesh.shape["node"]), ALL)
    placed = (
        P("node", SEC, None, None),
        P("node", SEC, None, None),
        P("node", SEC),
        P("node", None),
        P("node", SEC),
    )
    return jax.shard_map(
        body, mesh=split, in_specs=placed, out_specs=P("node", SEC, None, None), check_vma=False
    )
```

```python
import functools

import jax
import jax.numpy as jnp
from jax import lax
from jax.experimental import pallas as pl
from jax.experimental.pallas import tpu as pltpu
from jax.sharding import Mesh
from jax.sharding import PartitionSpec as P

SEC = ("x", "y_hi", "y_lo", "z")
ALL = SEC + ("node",)
FAMILY = ("y_lo", "z", "node")
LOCAL = 8
DC = 128
HALF = 64
SLOTS = 384
CHUNK = 64
CHUNKS = SLOTS // CHUNK
PIECE = 40
F32 = jnp.float32


def rows_and_lanes(rows):
    row = lax.broadcasted_iota(jnp.int32, (rows, DC), 0)
    lane = lax.broadcasted_iota(jnp.int32, (rows, DC), 1)
    return row, lane


def partial_sums(
    live_ref, joined_hbm, owner_hbm, env, iso, out_ref, sector_ref,
    e_buf, w_buf, acc, joined_ref, owner_ref, e_sem, w_sem, small_sem,
):
    small = [
        pltpu.make_async_copy(source, target, small_sem.at[i])
        for i, (source, target) in enumerate(
            ((joined_hbm, joined_ref), (owner_hbm, owner_ref))
        )
    ]
    for copy in small:
        copy.start()

    def copies(chunk):
        here = pl.ds(chunk * CHUNK, CHUNK)
        return (
            pltpu.make_async_copy(env.at[0, here], e_buf.at[here], e_sem.at[chunk]),
            pltpu.make_async_copy(iso.at[0, here], w_buf.at[here], w_sem.at[chunk]),
        )

    def start(chunk, carry):
        for copy in copies(chunk):
            copy.start()
        return carry

    live = live_ref[0, 0]
    chunks = (live + CHUNK - 1) // CHUNK
    lax.fori_loop(0, chunks, start, 0)
    acc[...] = jnp.zeros_like(acc)
    for copy in small:
        copy.wait()
    sec = (
        (lax.axis_index("x") * 2 + lax.axis_index("y_hi")) * 2 + lax.axis_index("y_lo")
    ) * 4 + lax.axis_index("z")
    sector = lax.fori_loop(
        0, 64, lambda d, found: jnp.where(owner_ref[0, d] == sec, d, found), jnp.int32(0)
    )
    sector_ref[...] = jnp.full((8, DC), sector, jnp.int32)

    def add_chunk(chunk, carry):
        for copy in copies(chunk):
            copy.wait()
        for u in range(CHUNK):
            slot = chunk * CHUNK + u
            weights = w_buf[slot]
            product = jnp.dot(e_buf[slot], weights, preferred_element_type=F32).astype(jnp.bfloat16)
            term = lax.dot_general(
                weights, product, (((0,), (0,)), ((), ())), preferred_element_type=F32
            )
            sector = jnp.where(slot < live, joined_ref[0, slot] & (LOCAL - 1), LOCAL)
            acc[sector] = acc[sector] + term
        return carry

    lax.fori_loop(0, chunks, add_chunk, 0)

    row, lane = rows_and_lanes(HALF)
    row8, lane8 = rows_and_lanes(8)
    family = 2 * lax.axis_index("x") + lax.axis_index("y_hi")
    packed, diagonals = [], []
    for j in range(LOCAL):
        top, bottom = acc[j, :HALF], acc[j, HALF:]
        turned = bottom.T[HALF:]
        turned = jnp.concatenate([turned, jnp.zeros_like(turned)], axis=1)
        packed.append(jnp.where(lane >= row, top, turned))
        diagonal = jnp.sum(jnp.where(lane == row + HALF, bottom, 0.0), axis=0, keepdims=True)
        owner = owner_ref[0, LOCAL * family + j].astype(F32)
        diagonals.append(jnp.where(lane8[:1] < HALF, owner, diagonal))
    diagonal_tile = jnp.concatenate(diagonals, axis=0)
    for v in range(8):
        rows = slice(8 * v, 8 * v + 8)
        for pair in range(LOCAL // 2):
            even, odd = packed[2 * pair][rows], packed[2 * pair + 1][rows]
            out_ref[2 * v, 8 * pair : 8 * pair + 8] = jnp.where(row8 < 4, even, odd)
            out_ref[2 * v + 1, 8 * pair : 8 * pair + 8] = jnp.where(row8 < 4, odd, even)
        out_ref[2 * v, 32:40] = diagonal_tile
        out_ref[2 * v + 1, 32:40] = diagonal_tile


def reduce_pieces(got_ref, out_ref):
    v = lax.axis_index("y_lo") * 4 + lax.axis_index("z")
    h = lax.axis_index("node")
    row, lane = rows_and_lanes(8)
    weight = jnp.where((lane < HALF) & (lane == row + 8 * v), 1.0, 2.0)
    first = HALF + 8 * v + 4 * h
    mine = (lane >= first) & (lane < first + 4)
    squares = jnp.zeros((8, DC), F32)
    summed = []
    for n in range(2):
        tiles = []
        for t in range(5):
            rows = slice(8 * t, 8 * t + 8)
            total = got_ref[n, rows]
            for source in range(1, 8):
                total = total + got_ref[2 * source + n, rows]
            tiles.append(total)
            squares = squares + jnp.where(mine, total * total, 0.0) if t == 4 else squares + weight * (total * total)
        summed.append(tiles)
    part = jnp.sum(squares)
    out_ref[...] = jnp.zeros_like(out_ref)
    out_ref[:, 0, 512:640] = jnp.full((128, DC), part, F32)
    for n in range(2):
        extra = summed[n][4]
        owners = (extra[:, :1] * 0.125).astype(jnp.int32)
        for j in range(LOCAL):
            slot = 2 * owners[j, 0] + n
            tile = summed[n][j // 2]
            low, high = tile[:4], tile[4:]
            mine4 = jnp.where(h == j % 2, low, high)
            for r in range(4):
                out_ref[slot, :, DC * r : DC * (r + 1)] = mine4[r : r + 1]
            out_ref[slot, :, 512:640] = jnp.where(lane[:1] < HALF, part, extra[j : j + 1])


def unpack(sector_ref, got_ref, out_ref, rows_buf):
    sector = sector_ref[:1, :1][0, 0]
    base = 16 * (sector // LOCAL)
    odd = sector % 2
    for v in range(8):
        for half in range(2):
            source = base + 2 * v + jnp.where(odd == 0, half, 1 - half)
            for r in range(4):
                rows_buf[8 * v + 4 * half + r : 8 * v + 4 * half + r + 1, :] = got_ref[
                    source, :, DC * r : DC * (r + 1)
                ]
    rows_buf[HALF:, :] = jnp.zeros((HALF, DC), F32)
    extra = got_ref[base, :, 512:640]
    total = jnp.sum(got_ref[:, 0, 512:640], axis=0, keepdims=True)[:, :1]
    factor = lax.rsqrt(total / (2 * 64 * DC * DC) + 1e-06)
    row, lane = rows_and_lanes(HALF)
    packed = rows_buf[:HALF, :]
    turned = rows_buf[...].T
    top = jnp.where(lane >= row, packed, turned[:HALF])
    inner = pltpu.roll(jnp.where(lane < row, packed, turned[:HALF]), HALF, 1)
    inner = jnp.where(lane == row + HALF, extra, inner)
    bottom = jnp.where(lane < HALF, turned[HALF:], inner)
    out_ref[0, 0, :HALF, :] = top * factor
    out_ref[0, 0, HALF:, :] = bottom * factor


def body(env_blocks, iso_blocks, joined_sector, owner_map, live_pairs):
    smem = pl.BlockSpec(memory_space=pltpu.SMEM)
    vmem = pl.BlockSpec(memory_space=pltpu.VMEM)
    hbm = pl.BlockSpec(memory_space=pltpu.HBM)
    pieces, sector = pl.pallas_call(
        partial_sums,
        in_specs=[smem] + [hbm] * 4,
        out_specs=[vmem, vmem],
        out_shape=[
            jax.ShapeDtypeStruct((16, PIECE, DC), F32),
            jax.ShapeDtypeStruct((8, DC), jnp.int32),
        ],
        scratch_shapes=[
            pltpu.VMEM((SLOTS, DC, DC), jnp.bfloat16),
            pltpu.VMEM((SLOTS, DC, DC), jnp.bfloat16),
            pltpu.VMEM((LOCAL + 1, DC, DC), F32),
            pltpu.SMEM((1, SLOTS), jnp.int32),
            pltpu.SMEM((1, 64), jnp.int32),
            pltpu.SemaphoreType.DMA((CHUNKS,)),
            pltpu.SemaphoreType.DMA((CHUNKS,)),
            pltpu.SemaphoreType.DMA((2,)),
        ],
        compiler_params=pltpu.CompilerParams(vmem_limit_bytes=48 << 20),
        name="partial_sums",
    )(
        live_pairs,
        pltpu.with_memory_space_constraint(joined_sector, pltpu.HBM),
        pltpu.with_memory_space_constraint(owner_map, pltpu.HBM),
        env_blocks,
        iso_blocks,
    )
    pieces = lax.all_to_all(pieces, FAMILY, 0, 0, tiled=True)
    slots = pl.pallas_call(
        reduce_pieces,
        in_specs=[vmem],
        out_specs=vmem,
        out_shape=jax.ShapeDtypeStruct((128, 1, 640), F32),
        compiler_params=pltpu.CompilerParams(vmem_limit_bytes=8 << 20),
        name="reduce_pieces",
    )(pieces)
    slots = lax.all_to_all(slots, ALL, 0, 0, tiled=True)
    return pl.pallas_call(
        unpack,
        in_specs=[vmem, vmem],
        out_specs=vmem,
        out_shape=jax.ShapeDtypeStruct((1, 1, DC, DC), F32),
        scratch_shapes=[pltpu.VMEM((DC, DC), F32)],
        compiler_params=pltpu.CompilerParams(vmem_limit_bytes=8 << 20),
        name="unpack",
    )(sector, slots)


def solution(mesh):
    split = Mesh(mesh.devices.reshape(4, 2, 2, 4, mesh.shape["node"]), ALL)
    placed = (
        P("node", SEC, None, None),
        P("node", SEC, None, None),
        P("node", SEC),
        P("node", None),
        P("node", SEC),
    )
    return jax.shard_map(
        body, mesh=split, in_specs=placed, out_specs=P("node", SEC, None, None), check_vma=False
    )
```

```python
import functools

import jax
import jax.numpy as jnp
from jax import lax
from jax.experimental import pallas as pl
from jax.experimental.pallas import tpu as pltpu
from jax.sharding import Mesh
from jax.sharding import PartitionSpec as P

SEC = ("x", "y_hi", "y_lo", "z")
ALL = SEC + ("node",)
FAMILY = ("y_lo", "z", "node")
LOCAL = 8
DC = 128
HALF = 64
SLOTS = 384
CHUNK = 64
CHUNKS = SLOTS // CHUNK
PIECE = 40
F32 = jnp.float32


def rows_and_lanes(rows):
    row = lax.broadcasted_iota(jnp.int32, (rows, DC), 0)
    lane = lax.broadcasted_iota(jnp.int32, (rows, DC), 1)
    return row, lane


def partial_sums(
    live_ref, joined_hbm, owner_hbm, env, iso, out_ref, sector_ref,
    e_buf, w_buf, acc, joined_ref, owner_ref, e_sem, w_sem, small_sem,
):
    small = [
        pltpu.make_async_copy(source, target, small_sem.at[i])
        for i, (source, target) in enumerate(
            ((joined_hbm, joined_ref), (owner_hbm, owner_ref))
        )
    ]
    for copy in small:
        copy.start()

    def copies(chunk):
        here = pl.ds(chunk * CHUNK, CHUNK)
        return (
            pltpu.make_async_copy(env.at[0, here], e_buf.at[here], e_sem.at[chunk]),
            pltpu.make_async_copy(iso.at[0, here], w_buf.at[here], w_sem.at[chunk]),
        )

    def start(chunk, carry):
        for queue, copy in enumerate(copies(chunk)):
            copy.start(priority=queue)
        return carry

    live = live_ref[0, 0]
    chunks = (live + CHUNK - 1) // CHUNK
    lax.fori_loop(0, chunks, start, 0)
    acc[...] = jnp.zeros_like(acc)
    for copy in small:
        copy.wait()
    sec = (
        (lax.axis_index("x") * 2 + lax.axis_index("y_hi")) * 2 + lax.axis_index("y_lo")
    ) * 4 + lax.axis_index("z")
    sector = lax.fori_loop(
        0, 64, lambda d, found: jnp.where(owner_ref[0, d] == sec, d, found), jnp.int32(0)
    )
    sector_ref[...] = jnp.full((8, DC), sector, jnp.int32)

    def add_chunk(chunk, carry):
        for copy in copies(chunk):
            copy.wait()
        for u in range(CHUNK):
            slot = chunk * CHUNK + u
            weights = w_buf[slot]
            product = jnp.dot(e_buf[slot], weights, preferred_element_type=F32).astype(jnp.bfloat16)
            term = lax.dot_general(
                weights, product, (((0,), (0,)), ((), ())), preferred_element_type=F32
            )
            sector = jnp.where(slot < live, joined_ref[0, slot] & (LOCAL - 1), LOCAL)
            acc[sector] = acc[sector] + term
        return carry

    lax.fori_loop(0, chunks, add_chunk, 0)

    row, lane = rows_and_lanes(HALF)
    row8, lane8 = rows_and_lanes(8)
    family = 2 * lax.axis_index("x") + lax.axis_index("y_hi")
    packed, diagonals = [], []
    for j in range(LOCAL):
        top, bottom = acc[j, :HALF], acc[j, HALF:]
        turned = bottom.T[HALF:]
        turned = jnp.concatenate([turned, jnp.zeros_like(turned)], axis=1)
        packed.append(jnp.where(lane >= row, top, turned))
        diagonal = jnp.sum(jnp.where(lane == row + HALF, bottom, 0.0), axis=0, keepdims=True)
        owner = owner_ref[0, LOCAL * family + j].astype(F32)
        diagonals.append(jnp.where(lane8[:1] < HALF, owner, diagonal))
    diagonal_tile = jnp.concatenate(diagonals, axis=0)
    for v in range(8):
        rows = slice(8 * v, 8 * v + 8)
        for pair in range(LOCAL // 2):
            even, odd = packed[2 * pair][rows], packed[2 * pair + 1][rows]
            out_ref[2 * v, 8 * pair : 8 * pair + 8] = jnp.where(row8 < 4, even, odd)
            out_ref[2 * v + 1, 8 * pair : 8 * pair + 8] = jnp.where(row8 < 4, odd, even)
        out_ref[2 * v, 32:40] = diagonal_tile
        out_ref[2 * v + 1, 32:40] = diagonal_tile


def reduce_pieces(got_ref, out_ref):
    v = lax.axis_index("y_lo") * 4 + lax.axis_index("z")
    h = lax.axis_index("node")
    row, lane = rows_and_lanes(8)
    weight = jnp.where((lane < HALF) & (lane == row + 8 * v), 1.0, 2.0)
    first = HALF + 8 * v + 4 * h
    mine = (lane >= first) & (lane < first + 4)
    squares = jnp.zeros((8, DC), F32)
    summed = []
    for n in range(2):
        tiles = []
        for t in range(5):
            rows = slice(8 * t, 8 * t + 8)
            total = got_ref[n, rows]
            for source in range(1, 8):
                total = total + got_ref[2 * source + n, rows]
            tiles.append(total)
            squares = squares + jnp.where(mine, total * total, 0.0) if t == 4 else squares + weight * (total * total)
        summed.append(tiles)
    part = jnp.sum(squares)
    out_ref[...] = jnp.zeros_like(out_ref)
    out_ref[:, 0, 512:640] = jnp.full((128, DC), part, F32)
    for n in range(2):
        extra = summed[n][4]
        owners = (extra[:, :1] * 0.125).astype(jnp.int32)
        for j in range(LOCAL):
            slot = 2 * owners[j, 0] + n
            tile = summed[n][j // 2]
            low, high = tile[:4], tile[4:]
            mine4 = jnp.where(h == j % 2, low, high)
            for r in range(4):
                out_ref[slot, :, DC * r : DC * (r + 1)] = mine4[r : r + 1]
            out_ref[slot, :, 512:640] = jnp.where(lane[:1] < HALF, part, extra[j : j + 1])


def unpack(sector_ref, got_ref, out_ref, rows_buf):
    sector = sector_ref[:1, :1][0, 0]
    base = 16 * (sector // LOCAL)
    odd = sector % 2
    for v in range(8):
        for half in range(2):
            source = base + 2 * v + jnp.where(odd == 0, half, 1 - half)
            for r in range(4):
                rows_buf[8 * v + 4 * half + r : 8 * v + 4 * half + r + 1, :] = got_ref[
                    source, :, DC * r : DC * (r + 1)
                ]
    rows_buf[HALF:, :] = jnp.zeros((HALF, DC), F32)
    extra = got_ref[base, :, 512:640]
    total = jnp.sum(got_ref[:, 0, 512:640], axis=0, keepdims=True)[:, :1]
    factor = lax.rsqrt(total / (2 * 64 * DC * DC) + 1e-06)
    row, lane = rows_and_lanes(HALF)
    packed = rows_buf[:HALF, :]
    turned = rows_buf[...].T
    top = jnp.where(lane >= row, packed, turned[:HALF])
    inner = pltpu.roll(jnp.where(lane < row, packed, turned[:HALF]), HALF, 1)
    inner = jnp.where(lane == row + HALF, extra, inner)
    bottom = jnp.where(lane < HALF, turned[HALF:], inner)
    out_ref[0, 0, :HALF, :] = top * factor
    out_ref[0, 0, HALF:, :] = bottom * factor


def body(env_blocks, iso_blocks, joined_sector, owner_map, live_pairs):
    smem = pl.BlockSpec(memory_space=pltpu.SMEM)
    vmem = pl.BlockSpec(memory_space=pltpu.VMEM)
    hbm = pl.BlockSpec(memory_space=pltpu.HBM)
    pieces, sector = pl.pallas_call(
        partial_sums,
        in_specs=[smem] + [hbm] * 4,
        out_specs=[vmem, vmem],
        out_shape=[
            jax.ShapeDtypeStruct((16, PIECE, DC), F32),
            jax.ShapeDtypeStruct((8, DC), jnp.int32),
        ],
        scratch_shapes=[
            pltpu.VMEM((SLOTS, DC, DC), jnp.bfloat16),
            pltpu.VMEM((SLOTS, DC, DC), jnp.bfloat16),
            pltpu.VMEM((LOCAL + 1, DC, DC), F32),
            pltpu.SMEM((1, SLOTS), jnp.int32),
            pltpu.SMEM((1, 64), jnp.int32),
            pltpu.SemaphoreType.DMA((CHUNKS,)),
            pltpu.SemaphoreType.DMA((CHUNKS,)),
            pltpu.SemaphoreType.DMA((2,)),
        ],
        compiler_params=pltpu.CompilerParams(vmem_limit_bytes=48 << 20),
        name="partial_sums",
    )(
        live_pairs,
        pltpu.with_memory_space_constraint(joined_sector, pltpu.HBM),
        pltpu.with_memory_space_constraint(owner_map, pltpu.HBM),
        env_blocks,
        iso_blocks,
    )
    pieces = lax.all_to_all(pieces, FAMILY, 0, 0, tiled=True)
    slots = pl.pallas_call(
        reduce_pieces,
        in_specs=[vmem],
        out_specs=vmem,
        out_shape=jax.ShapeDtypeStruct((128, 1, 640), F32),
        compiler_params=pltpu.CompilerParams(vmem_limit_bytes=8 << 20),
        name="reduce_pieces",
    )(pieces)
    slots = lax.all_to_all(slots, ALL, 0, 0, tiled=True)
    return pl.pallas_call(
        unpack,
        in_specs=[vmem, vmem],
        out_specs=vmem,
        out_shape=jax.ShapeDtypeStruct((1, 1, DC, DC), F32),
        scratch_shapes=[pltpu.VMEM((DC, DC), F32)],
        compiler_params=pltpu.CompilerParams(vmem_limit_bytes=8 << 20),
        name="unpack",
    )(sector, slots)


def solution(mesh):
    split = Mesh(mesh.devices.reshape(4, 2, 2, 4, mesh.shape["node"]), ALL)
    placed = (
        P("node", SEC, None, None),
        P("node", SEC, None, None),
        P("node", SEC),
        P("node", None),
        P("node", SEC),
    )
    return jax.shard_map(
        body, mesh=split, in_specs=placed, out_specs=P("node", SEC, None, None), check_vma=False
    )
```
